32 devices in a mesh: seq: 8 (over z, y), head: 4 (over x, core).
Axes of the slice: x: 2, y: 2, z: 4, core: 2. Of those that a mesh axis runs over, the one named last changes fastest.
Arguments:
- queries: bfloat16 [1024, 4096], P('seq', 'head'), may hold values from -12 to 12
- keys: bfloat16 [1024, 2048], P('seq', 'head'), may hold values from -12 to 12
- values: bfloat16 [1024, 2048], P('seq', 'head'), may hold values from -6 to 6
- block_order: int32 [16], replicated, may hold values from 0 to 15, each once
Outputs:
- attn: bfloat16 [1024, 4096], P(('seq', 'head'))
- lse: float32 [16, 1024], P('head', 'seq')
The draws below stay inside these ranges and needn't reach their ends.
Inputs may be any that keep to these rules, and one draw needn't show every extreme that they name: device-order block j (rows j * 64 to j * 64 + 63) holds sequence positions block_order[j] * 64 onward, in order.
All inputs are finite; a program needn't handle non-finite values.
Results may differ from the reference program's by a relative error of at most 0.006.
Values may be sent and summed in bfloat16 or wider, within the bound.
A program may use at most 128 MiB of HBM per device.

```python
import jax
import jax.numpy as jnp
from jax import lax

HQ = 16
KEY_VALUE_HEADS = 8
HEAD_SIZE = 256
S_DEV = 128
QUERY_GROUP = 2
BLK = 64
NB = 16
SEQUENCE_TOKENS = 1024
N_SEQ = 8


def draw_queries(key, part):
    base_offset = jax.random.truncated_normal(jax.random.fold_in(key, 1), -3.0, 3.0, (SEQUENCE_TOKENS, HQ * HEAD_SIZE), jnp.float32)
    return base_offset.astype(jnp.bfloat16)


def draw_keys(key, part):
    base_offset = jax.random.truncated_normal(jax.random.fold_in(key, 2), -3.0, 3.0, (SEQUENCE_TOKENS, KEY_VALUE_HEADS * HEAD_SIZE), jnp.float32)
    return base_offset.astype(jnp.bfloat16)


def level_of(stream_key, extent, shards, smallest, top_value):
    def one(axis_at, blocks):
        heights = jax.random.uniform(jax.random.fold_in(jax.random.fold_in(stream_key, 6), axis_at), (blocks,), jnp.float32, smallest / len(shards), top_value / len(shards))
        return jnp.repeat(jnp.exp(heights), extent[axis_at] // blocks).reshape((-1,) + (1,) * (len(extent) - axis_at - 1))

    factor_of = one(*shards[0])
    for cut in shards[1:]:
        factor_of = factor_of * one(*cut)
    return factor_of


def scatter_about(key, shape, spread, most, pieces=(), held_as=jnp.bfloat16):
    array = jax.random.normal(key, shape, jnp.float32) * spread
    if len(pieces) > 0:
        array = level_of(key, shape, pieces, -0.22, 0.18) * array
    return jnp.clip(array, min=-most, max=most).astype(held_as)


def setup_inputs(seed: int = 0) -> dict:
    key_of = jax.random.split(jax.random.key(seed), 5)
    queries = draw_queries(jax.random.fold_in(key_of[4], 71), 0)
    keys = draw_keys(jax.random.fold_in(key_of[4], 71), 0)
    values = scatter_about(key_of[2], (SEQUENCE_TOKENS, KEY_VALUE_HEADS * HEAD_SIZE), 1.0, 6.0, ((0, 8), (1, 4)))
    block_order = jax.random.permutation(key_of[3], NB).astype(jnp.int32)
    return {"queries": queries, "keys": keys, "values": values, "block_order": block_order}


def reference(queries, keys, values, block_order):
    rows = jnp.arange(SEQUENCE_TOKENS, dtype=jnp.int32)
    pos = (block_order[rows // BLK] * BLK + rows % BLK).astype(jnp.int32)
    query_head_count = queries.reshape(SEQUENCE_TOKENS, KEY_VALUE_HEADS, QUERY_GROUP, HEAD_SIZE)
    key_single = keys.reshape(SEQUENCE_TOKENS, KEY_VALUE_HEADS, HEAD_SIZE).astype(jnp.float32)
    value_single = values.reshape(SEQUENCE_TOKENS, KEY_VALUE_HEADS, HEAD_SIZE).astype(jnp.float32)
    scale = HEAD_SIZE ** -0.5

    def one_block(index):
        start = (index * S_DEV).astype(jnp.int32)
        query_block = lax.dynamic_slice_in_dim(query_head_count, start, S_DEV, 0).astype(jnp.float32)
        query_pos = lax.dynamic_slice_in_dim(pos, start, S_DEV, 0)
        scores = jnp.einsum('qhgd,khd->hgqk', query_block, key_single) * scale
        allowed = pos[None, :] <= query_pos[:, None]
        scores = jnp.where(allowed, scores, -1e30)
        row_max = jnp.max(scores, axis=-1)
        weights = jnp.where(allowed, jnp.exp(scores - row_max[..., None]), 0.0)
        total = jnp.sum(weights, axis=-1)
        rounded = lax.optimization_barrier(weights.astype(jnp.bfloat16))
        summed = jnp.einsum('hgqk,khd->qhgd', rounded.astype(jnp.float32), value_single)
        output = summed / jnp.transpose(total, (2, 0, 1))[..., None]
        return output.reshape(S_DEV, HQ * HEAD_SIZE).astype(jnp.bfloat16), (row_max + jnp.log(total)).reshape(HQ, S_DEV)

    outputs, sums = lax.map(one_block, jnp.arange(N_SEQ, dtype=jnp.int32))
    attn = outputs.reshape(SEQUENCE_TOKENS, HQ * HEAD_SIZE)
    lse = jnp.transpose(sums, (1, 0, 2)).reshape(HQ, SEQUENCE_TOKENS)
    return attn, lse
```

```python
import functools

import jax
import jax.numpy as jnp
from jax import lax
from jax.experimental import pallas as pl
from jax.experimental.pallas import tpu as pltpu
from jax.sharding import PartitionSpec as P

HEAD_SIZE = 256
QUERY_GROUP = 2
MASKED = -1e30
FLOOR = -1e20
MESH = pl.DeviceIdType.MESH


def loop(first, last, body):
    if last - first <= 8:
        for i in range(first, last):
            body(i)
    else:
        lax.fori_loop(first, last, lambda i, c: (body(i), c)[1], 0)


def kernel(
    n, nh, order, q_hbm, k_hbm, v_hbm, attn, lse,
    qbuf, qout, kvown, kvbuf, maxima, sums, accum, obuf, lse_tx, lse_rx,
    load_sem, z_send, y_send, kv_recv, q_sem, o_send, o_recv, l_sem,
):
    head_dim, group = HEAD_SIZE, QUERY_GROUP
    rows = k_hbm.shape[0]
    keep = rows // nh
    line = n // 2
    scale = head_dim ** (-0.5)
    me, h = lax.axis_index("seq"), lax.axis_index("head")
    p, y = me // 2, lax.rem(me, 2)
    mine = lax.rem(p, 2)
    mate_p = p + 1 - 2 * mine
    mate = mate_p * 2 + y
    across = p * 2 + 1 - y
    width = group * head_dim

    def far(k):
        if isinstance(k, int):
            q, bit = 0, 1
            while bit < line:
                b = lax.rem(p // bit, 2)
                q = q + bit * ((1 - b) if k & bit else b)
                bit *= 2
            return q
        q, bit = 0, 1
        while bit < line:
            b, c = lax.rem(p // bit, 2), lax.rem(k // bit, 2)
            q = q + bit * lax.rem(b + c, 2)
            bit *= 2
        return q

    def lanes(start, size):
        return pl.ds(pl.multiple_of(start, head_dim), size)

    loads = []

    def load(src, dst):
        c = pltpu.make_async_copy(src, dst, load_sem.at[len(loads)])
        c.start()
        loads.append(c)

    for i, src in enumerate((k_hbm, v_hbm)):
        load(src.at[:, lanes(mine * head_dim, head_dim)], kvbuf.at[me, i])
    for j in range(2):
        for i, src in enumerate((k_hbm, v_hbm)):
            load(src.at[:, lanes(j * head_dim, head_dim)], kvown.at[j, i])
    for g in range(group):
        load(q_hbm.at[:, lanes(((1 - mine) * group + g) * head_dim, head_dim)],
             qout.at[pl.ds(g * rows, rows)])
    for g in range(group):
        load(q_hbm.at[:, lanes((mine * group + g) * head_dim, head_dim)],
             qbuf.at[0, pl.ds(g * rows, rows)])

    barrier = pltpu.get_barrier_semaphore()

    def greet(s, hh):
        pl.semaphore_signal(barrier, inc=1, device_id=(s, hh), device_id_type=MESH)

    greet(across, h)
    loop(1, line, lambda k: greet(far(k) * 2 + y, h))
    for j in range(1, nh):
        greet(me, lax.rem(h + j, nh))
        greet(mate, lax.rem(h + j, nh))

    maxima[...] = jnp.full_like(maxima, FLOOR)
    sums[...] = jnp.zeros_like(sums)
    accum[...] = jnp.zeros_like(accum)

    pl.semaphore_wait(barrier, 1 + (line - 1) + 2 * (nh - 1))

    def y_copy(q):
        slot = q * 2 + y
        return pltpu.make_async_remote_copy(
            src_ref=kvbuf.at[slot], dst_ref=kvbuf.at[slot],
            send_sem=y_send.at[q], recv_sem=kv_recv.at[slot],
            device_id=(across, h), device_id_type=MESH)

    def z_copy(k):
        q = far(k)
        return pltpu.make_async_remote_copy(
            src_ref=kvown.at[lax.rem(q, 2)], dst_ref=kvbuf.at[me],
            send_sem=z_send.at[k], recv_sem=kv_recv.at[me],
            device_id=(q * 2 + y, h), device_id_type=MESH)

    def arrived(slot):
        pltpu.make_async_remote_copy(
            src_ref=kvbuf.at[slot], dst_ref=kvbuf.at[slot],
            send_sem=y_send.at[0], recv_sem=kv_recv.at[slot],
            device_id=(across, h), device_id_type=MESH).wait_recv()

    q_copy = pltpu.make_async_remote_copy(
        src_ref=qout, dst_ref=qbuf.at[1], send_sem=q_sem.at[0], recv_sem=q_sem.at[1],
        device_id=(mate, h), device_id_type=MESH)

    for c in loads[:2]:
        c.wait()
    y_copy(p).start()
    for c in loads[2:6]:
        c.wait()
    loop(1, line, lambda k: z_copy(line - k).start())
    for c in loads[6:]:
        c.wait()
    q_copy.start()

    row = lax.broadcasted_iota(jnp.int32, (rows, rows), 0)
    col = lax.broadcasted_iota(jnp.int32, (rows, rows), 1)
    per = order.shape[0] // n
    blk = rows // per

    def placed(index, s):
        out = index + order[s * per] * blk
        for b in range(1, per):
            out = jnp.where(index >= b * blk, index + (order[s * per + b] - b) * blk, out)
        return out

    query_pos = [placed(row, s) for s in (me, mate)]

    def attend(rs, slot):
        keys, values = kvbuf[slot, 0], kvbuf[slot, 1]
        scores = lax.dot_general(
            qbuf[rs], keys, (((1,), (1,)), ((), ())), preferred_element_type=jnp.float32) * scale
        allowed = placed(col, slot) <= query_pos[rs]
        scores = jnp.where(jnp.concatenate([allowed] * group, 0), scores, MASKED)
        before = maxima[rs]
        fresh = jnp.maximum(before, jnp.max(scores, axis=1, keepdims=True))
        weights = jnp.exp(scores - fresh)
        factor = jnp.exp(before - fresh)
        maxima[rs] = fresh
        sums[rs] = sums[rs] * factor + weights
        update = lax.dot_general(
            weights.astype(jnp.bfloat16), values, (((1,), (0,)), ((), ())),
            preferred_element_type=jnp.float32)
        accum[rs] = accum[rs] * jnp.concatenate([factor] * (head_dim // rows), 1) + update

    attend(0, me)
    arrived(across)
    attend(0, across)

    def step(k):
        q = far(line - k)
        slot = q * 2 + y
        arrived(slot)
        y_copy(q).start()
        attend(0, slot)

    def step_with_last(k):
        step(k)
        last = far(line - k + 1) * 2 + 1 - y
        arrived(last)
        attend(0, last)

    step(1)
    loop(2, line, step_with_last)
    q_copy.wait_recv()
    final = far(1) * 2 + 1 - y
    attend(1, me)
    attend(1, across)

    def catch_up(k):
        q = far(line - k)
        attend(1, q * 2 + y)
        attend(1, q * 2 + 1 - y)

    loop(1, line - 1, catch_up)
    attend(1, far(1) * 2 + y)
    arrived(final)

    def finish(rs):
        attend(rs, final)
        total = jnp.sum(sums[rs], axis=1, keepdims=True)
        out = (accum[rs] / total).astype(jnp.bfloat16)
        for g in range(group):
            obuf[rs, :, g * head_dim:(g + 1) * head_dim] = out[g * rows:(g + 1) * rows]
        return jnp.log(total) + maxima[rs]

    def put_lse(rs, full):
        for g in range(group):
            lse_tx[rs, g:g + 1, :] = jnp.transpose(full[g * rows:(g + 1) * rows])[:1]

    columns = lanes((h * 2 + mine) * width, width)

    def o_copy(rs, j):
        to = lax.rem(h + j, nh)
        return pltpu.make_async_remote_copy(
            src_ref=obuf.at[rs, pl.ds(pl.multiple_of(to * keep, keep), keep)],
            dst_ref=attn.at[:, columns],
            send_sem=o_send.at[rs, j], recv_sem=o_recv.at[rs, h],
            device_id=((me, mate)[rs], to), device_id_type=MESH)

    outs = []
    full = finish(1)
    for j in range(nh):
        outs.append(o_copy(1, j))
        outs[-1].start()
    put_lse(1, full)
    lse_copy = pltpu.make_async_remote_copy(
        src_ref=lse_tx.at[1], dst_ref=lse_rx, send_sem=l_sem.at[0], recv_sem=l_sem.at[1],
        device_id=(mate, h), device_id_type=MESH)
    lse_copy.start()
    full = finish(0)
    for j in range(1, nh):
        outs.append(o_copy(0, j))
        outs[-1].start()
    kept = pltpu.make_async_copy(
        obuf.at[0, pl.ds(pl.multiple_of(h * keep, keep), keep)], attn.at[:, columns],
        o_send.at[0, 0])
    kept.start()
    put_lse(0, full)

    lse_copy.wait_recv()
    own, other = lse_tx[0, :group], lse_rx[:group]
    low = jnp.where(mine == 0, own, other)
    high = jnp.where(mine == 0, other, own)
    lse[...] = jnp.concatenate([low, high], 0)

    for rs in range(2):
        for j in range(1 - rs, nh):
            source = lax.rem(h + j, nh)
            spot = lanes((source * 2 + (mine, 1 - mine)[rs]) * width, width)
            pltpu.make_async_remote_copy(
                src_ref=obuf.at[rs, pl.ds(0, keep)], dst_ref=attn.at[:, spot],
                send_sem=o_send.at[rs, j], recv_sem=o_recv.at[rs, source],
                device_id=(mate, h), device_id_type=MESH).wait_recv()
    kept.wait()
    for c in outs:
        c.wait_send()
    lse_copy.wait_send()
    q_copy.wait_send()
    y_copy(p).wait_send()
    loop(1, line, lambda k: (z_copy(k).wait_send(), y_copy(far(k)).wait_send()))


def local(n, nh, queries, keys, values, block_order):
    rows = queries.shape[0]
    head_dim, group = HEAD_SIZE, QUERY_GROUP
    line = n // 2
    high = group * rows
    bf16, f32 = jnp.bfloat16, jnp.float32
    dma = pltpu.SemaphoreType.DMA
    return pl.pallas_call(
        functools.partial(kernel, n, nh),
        out_shape=(
            jax.ShapeDtypeStruct((rows // nh, queries.shape[1] * nh), bf16),
            jax.ShapeDtypeStruct((2 * group, rows), f32),
        ),
        in_specs=[pl.BlockSpec(memory_space=pltpu.SMEM)] + [pl.BlockSpec(memory_space=pl.ANY)] * 3,
        out_specs=(pl.BlockSpec(memory_space=pl.ANY), pl.BlockSpec(memory_space=pltpu.VMEM)),
        scratch_shapes=[
            pltpu.VMEM((2, high, head_dim), bf16),
            pltpu.VMEM((high, head_dim), bf16),
            pltpu.VMEM((2, 2, rows, head_dim), bf16),
            pltpu.VMEM((n, 2, rows, head_dim), bf16),
            pltpu.VMEM((2, high, rows), f32),
            pltpu.VMEM((2, high, rows), f32),
            pltpu.VMEM((2, high, head_dim), f32),
            pltpu.VMEM((2, rows, group * head_dim), bf16),
            pltpu.VMEM((2, 8, rows), f32),
            pltpu.VMEM((8, rows), f32),
            dma((6 + 2 * group,)),
            dma((line,)),
            dma((line,)),
            dma((n,)),
            dma((2,)),
            dma((2, nh)),
            dma((2, nh)),
            dma((2,)),
        ],
        compiler_params=pltpu.CompilerParams(collective_id=0, has_side_effects=True),
    )(block_order, queries, keys, values)


def solution(mesh):
    in_specs = (P("seq", "head"), P("seq", "head"), P("seq", "head"), P())
    out_specs = (P(("seq", "head"), None), P("head", "seq"))
    body = functools.partial(local, mesh.shape["seq"], mesh.shape["head"])
    return jax.shard_map(body, mesh=mesh, in_specs=in_specs, out_specs=out_specs, check_vma=False)
```

```python
import functools

import jax
import jax.numpy as jnp
from jax import lax
from jax.experimental import pallas as pl
from jax.experimental.pallas import tpu as pltpu
from jax.sharding import PartitionSpec as P

HEAD_SIZE = 256
QUERY_GROUP = 2
MASKED = -1e30
FLOOR = -1e20
PARTS = 2
MESH = pl.DeviceIdType.MESH


def loop(first, last, body):
    if last - first <= 8:
        for i in range(first, last):
            body(i)
    else:
        lax.fori_loop(first, last, lambda i, c: (body(i), c)[1], 0)


def kernel(
    n, nh, order, q_hbm, k_hbm, v_hbm, attn, lse,
    qbuf, qout, kvown, kvbuf, maxima, sums, accum, obuf, lse_tx, lse_rx,
    load_sem, z_send, y_send, kv_recv, q_sem, o_send, o_recv, l_sem,
):
    head_dim, group = HEAD_SIZE, QUERY_GROUP
    rows = k_hbm.shape[0]
    keep = rows // nh
    part = rows // PARTS
    line = n // 2
    scale = head_dim ** (-0.5)
    me, h = lax.axis_index("seq"), lax.axis_index("head")
    p, y = me // 2, lax.rem(me, 2)
    mine = lax.rem(p, 2)
    mate_p = p + 1 - 2 * mine
    mate = mate_p * 2 + y
    across = p * 2 + 1 - y
    width = group * head_dim

    core = lax.rem(h, 2)

    def far(k):
        q, bit = 0, 1
        while bit < line:
            b, c = lax.rem(p // bit, 2), (k // bit) % 2
            q = q + bit * (b + c - 2 * b * c)
            bit *= 2
        return q

    def turn(i):
        return jnp.where(core == 0, line - i, jnp.where(jnp.int32(i) == 1, 1, line - i + 1))

    def lanes(start, size):
        return pl.ds(pl.multiple_of(start, head_dim), size)

    loads = []

    def load(src, dst):
        c = pltpu.make_async_copy(src, dst, load_sem.at[len(loads)])
        c.start()
        loads.append(c)

    for i, src in enumerate((k_hbm, v_hbm)):
        for t in range(PARTS):
            load(src.at[pl.ds(t * part, part), lanes(mine * head_dim, head_dim)],
                 kvbuf.at[me, t, i])
    for j in range(2):
        for i, src in enumerate((k_hbm, v_hbm)):
            for t in range(PARTS):
                load(src.at[pl.ds(t * part, part), lanes(j * head_dim, head_dim)],
                     kvown.at[j, t, i])
    for g in range(group):
        load(q_hbm.at[:, lanes(((1 - mine) * group + g) * head_dim, head_dim)],
             qout.at[pl.ds(g * rows, rows)])
    for g in range(group):
        load(q_hbm.at[:, lanes((mine * group + g) * head_dim, head_dim)],
             qbuf.at[0, pl.ds(g * rows, rows)])

    barrier = pltpu.get_barrier_semaphore()

    def greet(s, hh):
        pl.semaphore_signal(barrier, inc=1, device_id=(s, hh), device_id_type=MESH)

    greet(across, h)
    loop(1, line, lambda k: greet(far(k) * 2 + y, h))
    for j in range(1, nh):
        greet(me, lax.rem(h + j, nh))
        greet(mate, lax.rem(h + j, nh))

    maxima[...] = jnp.full_like(maxima, FLOOR)
    sums[...] = jnp.zeros_like(sums)
    accum[...] = jnp.zeros_like(accum)

    pl.semaphore_wait(barrier, 1 + (line - 1) + 2 * (nh - 1))

    def y_copy(q, t):
        slot = q * 2 + y
        return pltpu.make_async_remote_copy(
            src_ref=kvbuf.at[slot, t], dst_ref=kvbuf.at[slot, t],
            send_sem=y_send.at[q, t], recv_sem=kv_recv.at[slot, t],
            device_id=(across, h), device_id_type=MESH)

    def z_copy(k, t):
        q = far(k)
        return pltpu.make_async_remote_copy(
            src_ref=kvown.at[lax.rem(q, 2), t], dst_ref=kvbuf.at[me, t],
            send_sem=z_send.at[k, t], recv_sem=kv_recv.at[me, t],
            device_id=(q * 2 + y, h), device_id_type=MESH)

    def landed(slot, t):
        pltpu.make_async_remote_copy(
            src_ref=kvbuf.at[slot, t], dst_ref=kvbuf.at[slot, t],
            send_sem=y_send.at[0, t], recv_sem=kv_recv.at[slot, t],
            device_id=(across, h), device_id_type=MESH).wait_recv()

    def arrived(slot):
        for t in range(PARTS):
            landed(slot, t)

    q_copy = pltpu.make_async_remote_copy(
        src_ref=qout, dst_ref=qbuf.at[1], send_sem=q_sem.at[0], recv_sem=q_sem.at[1],
        device_id=(mate, h), device_id_type=MESH)

    for c in loads[:2 * PARTS]:
        c.wait()
    for t in range(PARTS):
        y_copy(p, t).start()
    for c in loads[2 * PARTS:]:
        c.wait()

    def send(i):
        for t in range(PARTS):
            z_copy(turn(i), t).start()

    send(1)

    @pl.when(core == 1)
    def _():
        q_copy.start()

    loop(2, line, send)

    @pl.when(core == 0)
    def _():
        q_copy.start()

    row = lax.broadcasted_iota(jnp.int32, (rows, rows), 0)
    col = lax.broadcasted_iota(jnp.int32, (rows, rows), 1)
    per = order.shape[0] // n
    blk = rows // per

    def placed(index, s):
        out = index + order[s * per] * blk
        for b in range(1, per):
            out = jnp.where(index >= b * blk, index + (order[s * per + b] - b) * blk, out)
        return out

    query_pos = [placed(row, s) for s in (me, mate)]

    def attend(rs, slot):
        keys, values = kvbuf[slot, :, 0], kvbuf[slot, :, 1]
        keys, values = (z.reshape(rows, head_dim) for z in (keys, values))
        scores = lax.dot_general(
            qbuf[rs], keys, (((1,), (1,)), ((), ())), preferred_element_type=jnp.float32) * scale
        allowed = placed(col, slot) <= query_pos[rs]
        scores = jnp.where(jnp.concatenate([allowed] * group, 0), scores, MASKED)
        before = maxima[rs]
        fresh = jnp.maximum(before, jnp.max(scores, axis=1, keepdims=True))
        weights = jnp.exp(scores - fresh)
        factor = jnp.exp(before - fresh)
        maxima[rs] = fresh
        sums[rs] = sums[rs] * factor + weights
        update = lax.dot_general(
            weights.astype(jnp.bfloat16), values, (((1,), (0,)), ((), ())),
            preferred_element_type=jnp.float32)
        accum[rs] = accum[rs] * jnp.concatenate([factor] * (head_dim // rows), 1) + update

    attend(0, me)
    arrived(across)
    attend(0, across)

    def step(i):
        q = far(turn(i))
        slot = q * 2 + y
        for t in range(PARTS):
            landed(slot, t)
            y_copy(q, t).start()
        attend(0, slot)

    def step_with_last(i):
        step(i)
        last = far(turn(i - 1)) * 2 + 1 - y
        arrived(last)
        attend(0, last)

    step(1)
    loop(2, line, step_with_last)
    q_copy.wait_recv()
    attend(1, me)
    attend(1, across)

    def catch_up(i):
        q = far(turn(i))
        attend(1, q * 2 + y)
        attend(1, q * 2 + 1 - y)

    loop(1, line - 1, catch_up)
    end = far(turn(line - 1))
    attend(1, end * 2 + y)
    final = end * 2 + 1 - y
    arrived(final)

    def finish(rs):
        attend(rs, final)
        total = jnp.sum(sums[rs], axis=1, keepdims=True)
        out = (accum[rs] / total).astype(jnp.bfloat16)
        for g in range(group):
            obuf[rs, :, g * head_dim:(g + 1) * head_dim] = out[g * rows:(g + 1) * rows]
        return jnp.log(total) + maxima[rs]

    def put_lse(rs, full):
        for g in range(group):
            lse_tx[rs, g:g + 1, :] = jnp.transpose(full[g * rows:(g + 1) * rows])[:1]

    columns = lanes((h * 2 + mine) * width, width)

    def o_copy(rs, j):
        to = lax.rem(h + j, nh)
        return pltpu.make_async_remote_copy(
            src_ref=obuf.at[rs, pl.ds(pl.multiple_of(to * keep, keep), keep)],
            dst_ref=attn.at[:, columns],
            send_sem=o_send.at[rs, j], recv_sem=o_recv.at[rs, h],
            device_id=((me, mate)[rs], to), device_id_type=MESH)

    outs = []
    full = finish(1)
    for j in range(nh):
        outs.append(o_copy(1, j))
        outs[-1].start()
    put_lse(1, full)
    lse_copy = pltpu.make_async_remote_copy(
        src_ref=lse_tx.at[1], dst_ref=lse_rx, send_sem=l_sem.at[0], recv_sem=l_sem.at[1],
        device_id=(mate, h), device_id_type=MESH)
    lse_copy.start()
    full = finish(0)
    for j in range(1, nh):
        outs.append(o_copy(0, j))
        outs[-1].start()
    kept = pltpu.make_async_copy(
        obuf.at[0, pl.ds(pl.multiple_of(h * keep, keep), keep)], attn.at[:, columns],
        o_send.at[0, 0])
    kept.start()
    put_lse(0, full)

    lse_copy.wait_recv()
    own, other = lse_tx[0, :group], lse_rx[:group]
    low = jnp.where(mine == 0, own, other)
    high = jnp.where(mine == 0, other, own)
    lse[...] = jnp.concatenate([low, high], 0)

    for rs in range(2):
        for j in range(1 - rs, nh):
            source = lax.rem(h + j, nh)
            spot = lanes((source * 2 + (mine, 1 - mine)[rs]) * width, width)
            pltpu.make_async_remote_copy(
                src_ref=obuf.at[rs, pl.ds(0, keep)], dst_ref=attn.at[:, spot],
                send_sem=o_send.at[rs, j], recv_sem=o_recv.at[rs, source],
                device_id=(mate, h), device_id_type=MESH).wait_recv()
    kept.wait()
    for c in outs:
        c.wait_send()
    lse_copy.wait_send()
    q_copy.wait_send()
    for t in range(PARTS):
        y_copy(p, t).wait_send()
        loop(1, line, lambda k: (z_copy(k, t).wait_send(), y_copy(far(k), t).wait_send()))


def local(n, nh, queries, keys, values, block_order):
    rows = queries.shape[0]
    head_dim, group = HEAD_SIZE, QUERY_GROUP
    line = n // 2
    high = group * rows
    bf16, f32 = jnp.bfloat16, jnp.float32
    dma = pltpu.SemaphoreType.DMA
    return pl.pallas_call(
        functools.partial(kernel, n, nh),
        out_shape=(
            jax.ShapeDtypeStruct((rows // nh, queries.shape[1] * nh), bf16),
            jax.ShapeDtypeStruct((2 * group, rows), f32),
        ),
        in_specs=[pl.BlockSpec(memory_space=pltpu.SMEM)] + [pl.BlockSpec(memory_space=pltpu.MemorySpace.HBM)] * 3,
        out_specs=(pl.BlockSpec(memory_space=pl.ANY), pl.BlockSpec(memory_space=pltpu.VMEM)),
        scratch_shapes=[
            pltpu.VMEM((2, high, head_dim), bf16),
            pltpu.VMEM((high, head_dim), bf16),
            pltpu.VMEM((2, PARTS, 2, rows // PARTS, head_dim), bf16),
            pltpu.VMEM((n, PARTS, 2, rows // PARTS, head_dim), bf16),
            pltpu.VMEM((2, high, rows), f32),
            pltpu.VMEM((2, high, rows), f32),
            pltpu.VMEM((2, high, head_dim), f32),
            pltpu.VMEM((2, rows, group * head_dim), bf16),
            pltpu.VMEM((2, 8, rows), f32),
            pltpu.VMEM((8, rows), f32),
            dma((6 * PARTS + 2 * group,)),
            dma((line, PARTS)),
            dma((line, PARTS)),
            dma((n, PARTS)),
            dma((2,)),
            dma((2, nh)),
            dma((2, nh)),
            dma((2,)),
        ],
        compiler_params=pltpu.CompilerParams(collective_id=0, has_side_effects=True),
    )(block_order, queries, keys, values)


def solution(mesh):
    in_specs = (P("seq", "head"), P("seq", "head"), P("seq", "head"), P())
    out_specs = (P(("seq", "head"), None), P("head", "seq"))
    body = functools.partial(local, mesh.shape["seq"], mesh.shape["head"])
    return jax.shard_map(body, mesh=mesh, in_specs=in_specs, out_specs=out_specs, check_vma=False)
```

```python
import functools

import jax
import jax.numpy as jnp
from jax import lax
from jax.experimental import pallas as pl
from jax.experimental.pallas import tpu as pltpu
from jax.sharding import PartitionSpec as P

HEAD_SIZE = 256
QUERY_GROUP = 2
MASKED = -1e30
FLOOR = -1e20
PARTS = 2
MESH = pl.DeviceIdType.MESH


def loop(first, last, body):
    if last - first <= 8:
        for i in range(first, last):
            body(i)
    else:
        lax.fori_loop(first, last, lambda i, c: (body(i), c)[1], 0)


def kernel(
    n, nh, order_hbm, q_hbm, k_hbm, v_hbm, attn, lse,
    qbuf, qout, kvown, kvbuf, maxima, sums, accum, obuf, lse_tx, lse_rx, lse_all, order,
    load_sem, z_send, y_send, kv_recv, q_sem, o_send, o_recv, l_sem,
):
    head_dim, group = HEAD_SIZE, QUERY_GROUP
    rows = k_hbm.shape[0]
    keep = rows // nh
    part = rows // PARTS
    line = n // 2
    scale = head_dim ** (-0.5)
    me, h = lax.axis_index("seq"), lax.axis_index("head")
    p, y = me // 2, lax.rem(me, 2)
    mine = lax.rem(p, 2)
    mate_p = p + 1 - 2 * mine
    mate = mate_p * 2 + y
    across = p * 2 + 1 - y
    width = group * head_dim

    core = lax.rem(h, 2)

    def far(k):
        q, bit = 0, 1
        while bit < line:
            b, c = lax.rem(p // bit, 2), (k // bit) % 2
            q = q + bit * (b + c - 2 * b * c)
            bit *= 2
        return q

    def turn(i):
        i = jnp.int32(i)
        second = jnp.where(i == 1, line - 1, jnp.where(i == 2, 1, line - i + 1))
        first = jnp.where(i == 1, 1, line - i + 1)
        return jnp.where(core == 0, second, first)

    def lanes(start, size):
        return pl.ds(pl.multiple_of(start, head_dim), size)

    loads = []

    def load(src, dst):
        c = pltpu.make_async_copy(src, dst, load_sem.at[len(loads)])
        c.start()
        loads.append(c)

    for i, src in enumerate((k_hbm, v_hbm)):
        for t in range(PARTS):
            load(src.at[pl.ds(t * part, part), lanes(mine * head_dim, head_dim)],
                 kvbuf.at[me, t, i])
    for j in range(2):
        for i, src in enumerate((k_hbm, v_hbm)):
            for t in range(PARTS):
                load(src.at[pl.ds(t * part, part), lanes(j * head_dim, head_dim)],
                     kvown.at[j, t, i])
    for g in range(group):
        load(q_hbm.at[:, lanes(((1 - mine) * group + g) * head_dim, head_dim)],
             qout.at[pl.ds(g * rows, rows)])
    for g in range(group):
        load(q_hbm.at[:, lanes((mine * group + g) * head_dim, head_dim)],
             qbuf.at[0, pl.ds(g * rows, rows)])

    load(order_hbm, order)

    barrier = pltpu.get_barrier_semaphore()

    def greet(s, hh):
        pl.semaphore_signal(barrier, inc=1, device_id=(s, hh), device_id_type=MESH)

    greet(across, h)
    loop(1, line, lambda k: greet(far(k) * 2 + y, h))
    for j in range(1, nh):
        greet(me, lax.rem(h + j, nh))
        greet(mate, lax.rem(h + j, nh))

    maxima[...] = jnp.full_like(maxima, FLOOR)
    sums[...] = jnp.zeros_like(sums)
    accum[...] = jnp.zeros_like(accum)

    pl.semaphore_wait(barrier, 1 + (line - 1) + 2 * (nh - 1))

    def y_copy(q, t):
        slot = q * 2 + y
        return pltpu.make_async_remote_copy(
            src_ref=kvbuf.at[slot, t], dst_ref=kvbuf.at[slot, t],
            send_sem=y_send.at[q, t], recv_sem=kv_recv.at[slot, t],
            device_id=(across, h), device_id_type=MESH)

    def z_copy(k, t):
        q = far(k)
        return pltpu.make_async_remote_copy(
            src_ref=kvown.at[lax.rem(q, 2), t], dst_ref=kvbuf.at[me, t],
            send_sem=z_send.at[k, t], recv_sem=kv_recv.at[me, t],
            device_id=(q * 2 + y, h), device_id_type=MESH)

    def landed(slot, t):
        pltpu.make_async_remote_copy(
            src_ref=kvbuf.at[slot, t], dst_ref=kvbuf.at[slot, t],
            send_sem=y_send.at[0, t], recv_sem=kv_recv.at[slot, t],
            device_id=(across, h), device_id_type=MESH).wait_recv()

    def arrived(slot):
        for t in range(PARTS):
            landed(slot, t)

    q_copy = pltpu.make_async_remote_copy(
        src_ref=qout, dst_ref=qbuf.at[1], send_sem=q_sem.at[0], recv_sem=q_sem.at[1],
        device_id=(mate, h), device_id_type=MESH)

    for c in loads[:2 * PARTS]:
        c.wait()
    for t in range(PARTS):
        y_copy(p, t).start()
    for c in loads[2 * PARTS:]:
        c.wait()

    def send(i):
        for t in range(PARTS):
            z_copy(turn(i), t).start()

    send(1)

    @pl.when(core == 1)
    def _():
        q_copy.start()

    loop(2, line, send)

    @pl.when(core == 0)
    def _():
        q_copy.start()

    row = lax.broadcasted_iota(jnp.int32, (rows, rows), 0)
    col = lax.broadcasted_iota(jnp.int32, (rows, rows), 1)
    per = order.shape[0] // n
    blk = rows // per

    def placed(index, s):
        out = index + order[s * per] * blk
        for b in range(1, per):
            out = jnp.where(index >= b * blk, index + (order[s * per + b] - b) * blk, out)
        return out

    query_pos = [placed(row, s) for s in (me, mate)]

    def attend(rs, slot):
        keys, values = kvbuf[slot, :, 0], kvbuf[slot, :, 1]
        keys, values = (z.reshape(rows, head_dim) for z in (keys, values))
        scores = lax.dot_general(
            qbuf[rs], keys, (((1,), (1,)), ((), ())), preferred_element_type=jnp.float32) * scale
        allowed = placed(col, slot) <= query_pos[rs]
        scores = jnp.where(jnp.concatenate([allowed] * group, 0), scores, MASKED)
        before = maxima[rs]
        fresh = jnp.maximum(before, jnp.max(scores, axis=1, keepdims=True))
        weights = jnp.exp(scores - fresh)
        factor = jnp.exp(before - fresh)
        maxima[rs] = fresh
        sums[rs] = sums[rs] * factor + weights
        update = lax.dot_general(
            weights.astype(jnp.bfloat16), values, (((1,), (0,)), ((), ())),
            preferred_element_type=jnp.float32)
        accum[rs] = accum[rs] * jnp.concatenate([factor] * (head_dim // rows), 1) + update

    attend(0, me)
    arrived(across)
    attend(0, across)

    def step(i):
        q = far(turn(i))
        slot = q * 2 + y
        for t in range(PARTS):
            landed(slot, t)
            y_copy(q, t).start()
        attend(0, slot)

    def step_with_last(i):
        step(i)
        last = far(turn(i - 1)) * 2 + 1 - y
        arrived(last)
        attend(0, last)

    step(1)
    loop(2, line, step_with_last)
    q_copy.wait_recv()
    attend(1, me)
    attend(1, across)

    def catch_up(i):
        q = far(turn(i))
        attend(1, q * 2 + y)
        attend(1, q * 2 + 1 - y)

    loop(1, line - 1, catch_up)
    end = far(turn(line - 1))
    attend(1, end * 2 + y)
    final = end * 2 + 1 - y
    arrived(final)

    def finish(rs):
        attend(rs, final)
        total = jnp.sum(sums[rs], axis=1, keepdims=True)
        out = (accum[rs] / total).astype(jnp.bfloat16)
        for g in range(group):
            obuf[rs, :, g * head_dim:(g + 1) * head_dim] = out[g * rows:(g + 1) * rows]
        return jnp.log(total) + maxima[rs]

    def put_lse(rs, full):
        for g in range(group):
            lse_tx[rs, g:g + 1, :] = jnp.transpose(full[g * rows:(g + 1) * rows])[:1]

    columns = lanes((h * 2 + mine) * width, width)

    def o_copy(rs, j):
        to = lax.rem(h + j, nh)
        return pltpu.make_async_remote_copy(
            src_ref=obuf.at[rs, pl.ds(pl.multiple_of(to * keep, keep), keep)],
            dst_ref=attn.at[:, columns],
            send_sem=o_send.at[rs, j], recv_sem=o_recv.at[rs, h],
            device_id=((me, mate)[rs], to), device_id_type=MESH)

    outs = []
    full = finish(1)
    for j in range(nh):
        outs.append(o_copy(1, j))
        outs[-1].start()
    put_lse(1, full)
    lse_copy = pltpu.make_async_remote_copy(
        src_ref=lse_tx.at[1], dst_ref=lse_rx, send_sem=l_sem.at[0], recv_sem=l_sem.at[1],
        device_id=(mate, h), device_id_type=MESH)
    lse_copy.start()
    full = finish(0)
    for j in range(1, nh):
        outs.append(o_copy(0, j))
        outs[-1].start()
    kept = pltpu.make_async_copy(
        obuf.at[0, pl.ds(pl.multiple_of(h * keep, keep), keep)], attn.at[:, columns],
        o_send.at[0, 0])
    kept.start()
    put_lse(0, full)

    lse_copy.wait_recv()
    own, other = lse_tx[0, :group], lse_rx[:group]
    low = jnp.where(mine == 0, own, other)
    high = jnp.where(mine == 0, other, own)
    lse_all[...] = jnp.concatenate([low, high], 0)
    lse_out = pltpu.make_async_copy(lse_all, lse, l_sem.at[2])
    lse_out.start()

    for rs in range(2):
        for j in range(1 - rs, nh):
            source = lax.rem(h + j, nh)
            spot = lanes((source * 2 + (mine, 1 - mine)[rs]) * width, width)
            pltpu.make_async_remote_copy(
                src_ref=obuf.at[rs, pl.ds(0, keep)], dst_ref=attn.at[:, spot],
                send_sem=o_send.at[rs, j], recv_sem=o_recv.at[rs, source],
                device_id=(mate, h), device_id_type=MESH).wait_recv()
    kept.wait()
    for c in outs:
        c.wait_send()
    lse_copy.wait_send()
    lse_out.wait()
    q_copy.wait_send()
    for t in range(PARTS):
        y_copy(p, t).wait_send()
        loop(1, line, lambda k: (z_copy(k, t).wait_send(), y_copy(far(k), t).wait_send()))


def local(n, nh, queries, keys, values, block_order):
    rows = queries.shape[0]
    head_dim, group = HEAD_SIZE, QUERY_GROUP
    line = n // 2
    high = group * rows
    bf16, f32 = jnp.bfloat16, jnp.float32
    dma = pltpu.SemaphoreType.DMA
    return pl.pallas_call(
        functools.partial(kernel, n, nh),
        out_shape=(
            jax.ShapeDtypeStruct((rows // nh, queries.shape[1] * nh), bf16),
            jax.ShapeDtypeStruct((2 * group, rows), f32),
        ),
        in_specs=[pl.BlockSpec(memory_space=pl.ANY)] * 4,
        out_specs=(pl.BlockSpec(memory_space=pl.ANY),) * 2,
        scratch_shapes=[
            pltpu.VMEM((2, high, head_dim), bf16),
            pltpu.VMEM((high, head_dim), bf16),
            pltpu.VMEM((2, PARTS, 2, rows // PARTS, head_dim), bf16),
            pltpu.VMEM((n, PARTS, 2, rows // PARTS, head_dim), bf16),
            pltpu.VMEM((2, high, rows), f32),
            pltpu.VMEM((2, high, rows), f32),
            pltpu.VMEM((2, high, head_dim), f32),
            pltpu.VMEM((2, rows, group * head_dim), bf16),
            pltpu.VMEM((2, 8, rows), f32),
            pltpu.VMEM((8, rows), f32),
            pltpu.VMEM((2 * group, rows), f32),
            pltpu.SMEM(block_order.shape, jnp.int32),
            dma((6 * PARTS + 2 * group + 1,)),
            dma((line, PARTS)),
            dma((line, PARTS)),
            dma((n, PARTS)),
            dma((2,)),
            dma((2, nh)),
            dma((2, nh)),
            dma((3,)),
        ],
        compiler_params=pltpu.CompilerParams(collective_id=0, has_side_effects=True),
    )(block_order, queries, keys, values)


def solution(mesh):
    in_specs = (P("seq", "head"), P("seq", "head"), P("seq", "head"), P())
    out_specs = (P(("seq", "head"), None), P("head", "seq"))
    body = functools.partial(local, mesh.shape["seq"], mesh.shape["head"])
    return jax.shard_map(body, mesh=mesh, in_specs=in_specs, out_specs=out_specs, check_vma=False)
```

```python
import functools

import jax
import jax.numpy as jnp
from jax import lax
from jax.experimental import pallas as pl
from jax.experimental.pallas import tpu as pltpu
from jax.sharding import PartitionSpec as P

HEAD_SIZE = 256
QUERY_GROUP = 2
MASKED = -1e30
FLOOR = -1e20
PARTS = 2
MESH = pl.DeviceIdType.MESH


def loop(first, last, body):
    if last - first <= 8:
        for i in range(first, last):
            body(i)
    else:
        lax.fori_loop(first, last, lambda i, c: (body(i), c)[1], 0)


def kernel(
    n, nh, order_hbm, q_hbm, k_hbm, v_hbm, attn, lse,
    qbuf, qout, kvown, kvbuf, maxima, sums, accum, obuf, lse_tx, lse_rx, order,
    load_sem, z_send, y_send, kv_recv, q_sem, o_send, o_recv, l_sem,
):
    head_dim, group = HEAD_SIZE, QUERY_GROUP
    rows = k_hbm.shape[0]
    keep = rows // nh
    part = rows // PARTS
    line = n // 2
    scale = head_dim ** (-0.5)
    me, h = lax.axis_index("seq"), lax.axis_index("head")
    p, y = me // 2, lax.rem(me, 2)
    mine = lax.rem(p, 2)
    mate_p = p + 1 - 2 * mine
    mate = mate_p * 2 + y
    across = p * 2 + 1 - y
    width = group * head_dim

    core = lax.rem(h, 2)

    def far(k):
        q, bit = 0, 1
        while bit < line:
            b, c = lax.rem(p // bit, 2), (k // bit) % 2
            q = q + bit * (b + c - 2 * b * c)
            bit *= 2
        return q

    def turn(i):
        i = jnp.int32(i)
        second = jnp.where(i == 1, line - 1, jnp.where(i == 2, 1, line - i + 1))
        return jnp.where(core == 0, second, i)

    def lanes(start, size):
        return pl.ds(pl.multiple_of(start, head_dim), size)

    loads = []

    def load(src, dst):
        c = pltpu.make_async_copy(src, dst, load_sem.at[len(loads)])
        c.start()
        loads.append(c)

    for i, src in enumerate((k_hbm, v_hbm)):
        for t in range(PARTS):
            load(src.at[pl.ds(t * part, part), lanes(mine * head_dim, head_dim)],
                 kvbuf.at[me, t, i])
    for j in range(2):
        for i, src in enumerate((k_hbm, v_hbm)):
            for t in range(PARTS):
                load(src.at[pl.ds(t * part, part), lanes(j * head_dim, head_dim)],
                     kvown.at[j, t, i])
    for g in range(group):
        load(q_hbm.at[:, lanes(((1 - mine) * group + g) * head_dim, head_dim)],
             qout.at[pl.ds(g * rows, rows)])
    for g in range(group):
        load(q_hbm.at[:, lanes((mine * group + g) * head_dim, head_dim)],
             qbuf.at[0, pl.ds(g * rows, rows)])

    load(order_hbm, order)

    barrier = pltpu.get_barrier_semaphore()

    def greet(s, hh):
        pl.semaphore_signal(barrier, inc=1, device_id=(s, hh), device_id_type=MESH)

    greet(across, h)
    loop(1, line, lambda k: greet(far(k) * 2 + y, h))
    for j in range(1, nh):
        greet(me, lax.rem(h + j, nh))
        greet(mate, lax.rem(h + j, nh))

    maxima[...] = jnp.full_like(maxima, FLOOR)
    sums[...] = jnp.zeros_like(sums)
    accum[...] = jnp.zeros_like(accum)

    pl.semaphore_wait(barrier, 1 + (line - 1) + 2 * (nh - 1))

    def y_copy(q, t):
        slot = q * 2 + y
        return pltpu.make_async_remote_copy(
            src_ref=kvbuf.at[slot, t], dst_ref=kvbuf.at[slot, t],
            send_sem=y_send.at[q, t], recv_sem=kv_recv.at[slot, t],
            device_id=(across, h), device_id_type=MESH)

    def z_copy(k, t):
        q = far(k)
        return pltpu.make_async_remote_copy(
            src_ref=kvown.at[lax.rem(q, 2), t], dst_ref=kvbuf.at[me, t],
            send_sem=z_send.at[k, t], recv_sem=kv_recv.at[me, t],
            device_id=(q * 2 + y, h), device_id_type=MESH)

    def landed(slot, t):
        pltpu.make_async_remote_copy(
            src_ref=kvbuf.at[slot, t], dst_ref=kvbuf.at[slot, t],
            send_sem=y_send.at[0, t], recv_sem=kv_recv.at[slot, t],
            device_id=(across, h), device_id_type=MESH).wait_recv()

    def arrived(slot):
        for t in range(PARTS):
            landed(slot, t)

    q_copy = pltpu.make_async_remote_copy(
        src_ref=qout, dst_ref=qbuf.at[1], send_sem=q_sem.at[0], recv_sem=q_sem.at[1],
        device_id=(mate, h), device_id_type=MESH)

    for c in loads[:2 * PARTS]:
        c.wait()
    for t in range(PARTS):
        y_copy(p, t).start()
    for c in loads[2 * PARTS:]:
        c.wait()

    def send(i):
        for t in range(PARTS):
            z_copy(turn(i), t).start()

    send(1)

    @pl.when(core == 1)
    def _():
        q_copy.start()

    loop(2, line, send)

    @pl.when(core == 0)
    def _():
        q_copy.start()

    row = lax.broadcasted_iota(jnp.int32, (rows, rows), 0)
    col = lax.broadcasted_iota(jnp.int32, (rows, rows), 1)
    per = order.shape[0] // n
    blk = rows // per

    def placed(index, s):
        out = index + order[s * per] * blk
        for b in range(1, per):
            out = jnp.where(index >= b * blk, index + (order[s * per + b] - b) * blk, out)
        return out

    query_pos = [placed(row, s) for s in (me, mate)]

    def attend(rs, slot):
        keys, values = kvbuf[slot, :, 0], kvbuf[slot, :, 1]
        keys, values = (z.reshape(rows, head_dim) for z in (keys, values))
        scores = lax.dot_general(
            qbuf[rs], keys, (((1,), (1,)), ((), ())), preferred_element_type=jnp.float32) * scale
        allowed = placed(col, slot) <= query_pos[rs]
        scores = jnp.where(jnp.concatenate([allowed] * group, 0), scores, MASKED)
        before = maxima[rs]
        fresh = jnp.maximum(before, jnp.max(scores, axis=1, keepdims=True))
        weights = jnp.exp(scores - fresh)
        factor = jnp.exp(before - fresh)
        maxima[rs] = fresh
        sums[rs] = sums[rs] * factor + weights
        update = lax.dot_general(
            weights.astype(jnp.bfloat16), values, (((1,), (0,)), ((), ())),
            preferred_element_type=jnp.float32)
        accum[rs] = accum[rs] * jnp.concatenate([factor] * (head_dim // rows), 1) + update

    attend(0, me)
    arrived(across)
    attend(0, across)

    def step(i):
        q = far(turn(i))
        slot = q * 2 + y
        for t in range(PARTS):
            landed(slot, t)
            y_copy(q, t).start()
        attend(0, slot)

    def step_with_last(i):
        step(i)
        last = far(turn(i - 1)) * 2 + 1 - y
        arrived(last)
        attend(0, last)

    step(1)
    loop(2, line, step_with_last)
    q_copy.wait_recv()
    attend(1, me)
    attend(1, across)

    def catch_up(i):
        q = far(turn(i))
        attend(1, q * 2 + y)
        attend(1, q * 2 + 1 - y)

    loop(1, line - 1, catch_up)
    end = far(turn(line - 1))
    attend(1, end * 2 + y)
    final = end * 2 + 1 - y
    arrived(final)

    def finish(rs):
        attend(rs, final)
        total = jnp.sum(sums[rs], axis=1, keepdims=True)
        out = (accum[rs] / total).astype(jnp.bfloat16)
        for g in range(group):
            obuf[rs, :, g * head_dim:(g + 1) * head_dim] = out[g * rows:(g + 1) * rows]
        return jnp.log(total) + maxima[rs]

    def put_lse(rs, full):
        for g in range(group):
            lse_tx[rs, g:g + 1, :] = jnp.transpose(full[g * rows:(g + 1) * rows])[:1]

    columns = lanes((h * 2 + mine) * width, width)

    def o_copy(rs, j):
        to = lax.rem(h + j, nh)
        return pltpu.make_async_remote_copy(
            src_ref=obuf.at[rs, pl.ds(pl.multiple_of(to * keep, keep), keep)],
            dst_ref=attn.at[:, columns],
            send_sem=o_send.at[rs, j], recv_sem=o_recv.at[rs, h],
            device_id=((me, mate)[rs], to), device_id_type=MESH)

    outs = []
    full = finish(1)
    for j in range(nh):
        outs.append(o_copy(1, j))
        outs[-1].start()
    put_lse(1, full)
    lse_copy = pltpu.make_async_remote_copy(
        src_ref=lse_tx.at[1], dst_ref=lse_rx, send_sem=l_sem.at[0], recv_sem=l_sem.at[1],
        device_id=(mate, h), device_id_type=MESH)
    lse_copy.start()
    full = finish(0)
    for j in range(1, nh):
        outs.append(o_copy(0, j))
        outs[-1].start()
    kept = pltpu.make_async_copy(
        obuf.at[0, pl.ds(pl.multiple_of(h * keep, keep), keep)], attn.at[:, columns],
        o_send.at[0, 0])
    kept.start()
    put_lse(0, full)

    lse_copy.wait_recv()
    own, other = lse_tx[0, :group], lse_rx[:group]
    low = jnp.where(mine == 0, own, other)
    high = jnp.where(mine == 0, other, own)
    lse[...] = jnp.concatenate([low, high], 0)

    for rs in range(2):
        for j in range(1 - rs, nh):
            source = lax.rem(h + j, nh)
            spot = lanes((source * 2 + (mine, 1 - mine)[rs]) * width, width)
            pltpu.make_async_remote_copy(
                src_ref=obuf.at[rs, pl.ds(0, keep)], dst_ref=attn.at[:, spot],
                send_sem=o_send.at[rs, j], recv_sem=o_recv.at[rs, source],
                device_id=(mate, h), device_id_type=MESH).wait_recv()
    kept.wait()
    for c in outs:
        c.wait_send()
    lse_copy.wait_send()
    q_copy.wait_send()
    for t in range(PARTS):
        y_copy(p, t).wait_send()
        loop(1, line, lambda k: (z_copy(k, t).wait_send(), y_copy(far(k), t).wait_send()))


def local(n, nh, queries, keys, values, block_order):
    rows = queries.shape[0]
    head_dim, group = HEAD_SIZE, QUERY_GROUP
    line = n // 2
    high = group * rows
    bf16, f32 = jnp.bfloat16, jnp.float32
    dma = pltpu.SemaphoreType.DMA
    return pl.pallas_call(
        functools.partial(kernel, n, nh),
        out_shape=(
            pltpu.VMEM((rows // nh, queries.shape[1] * nh), bf16),
            pltpu.VMEM((2 * group, rows), f32),
        ),
        in_specs=[pl.BlockSpec(memory_space=pl.ANY)] * 4,
        out_specs=(pl.BlockSpec(memory_space=pltpu.VMEM),) * 2,
        scratch_shapes=[
            pltpu.VMEM((2, high, head_dim), bf16),
            pltpu.VMEM((high, head_dim), bf16),
            pltpu.VMEM((2, PARTS, 2, rows // PARTS, head_dim), bf16),
            pltpu.VMEM((n, PARTS, 2, rows // PARTS, head_dim), bf16),
            pltpu.VMEM((2, high, rows), f32),
            pltpu.VMEM((2, high, rows), f32),
            pltpu.VMEM((2, high, head_dim), f32),
            pltpu.VMEM((2, rows, group * head_dim), bf16),
            pltpu.VMEM((2, 8, rows), f32),
            pltpu.VMEM((8, rows), f32),
            pltpu.SMEM(block_order.shape, jnp.int32),
            dma((6 * PARTS + 2 * group + 1,)),
            dma((line, PARTS)),
            dma((line, PARTS)),
            dma((n, PARTS)),
            dma((2,)),
            dma((2, nh)),
            dma((2, nh)),
            dma((2,)),
        ],
        compiler_params=pltpu.CompilerParams(collective_id=0, has_side_effects=True),
    )(block_order, queries, keys, values)


def solution(mesh):
    in_specs = (P("seq", "head"), P("seq", "head"), P("seq", "head"), P())
    out_specs = (P(("seq", "head"), None), P("head", "seq"))
    body = functools.partial(local, mesh.shape["seq"], mesh.shape["head"])
    return jax.shard_map(body, mesh=mesh, in_specs=in_specs, out_specs=out_specs, check_vma=False)
```
